512 devices in a mesh: clip: 8 (over z_hi, x), seq: 64 (over y, z_lo, core).
Axes of the slice: x: 4, y: 8, z: 8 (z_hi: 2, z_lo: 4; z = z_hi * 4 + z_lo), core: 2. Of those that a mesh axis runs over, the one named last changes fastest.
Arguments:
- spatial_saved: bfloat16 [3, 512, 256, 576], P(None, ('clip', 'seq')), parts along dimension 1, may hold values from -48 to 48
- hidden: bfloat16 [512, 256, 1152], P(('clip', 'seq')), parts along dimension 0, may hold values from -6 to 6
- temporal_out_grad: bfloat16 [512, 256, 576], P(('clip', 'seq')), parts along dimension 0, may hold values from -6 to 6
- stream_grad: bfloat16 [512, 256, 1152], P(('clip', 'seq')), parts along dimension 0, may hold values from -6 to 6
- modulation: float32 [1152], replicated, may hold values from -0.5 to 1
- temporal_weights: bfloat16 [1152, 1728], P('seq'), may hold values from -0.1875 to 0.1875
- spatial_weights: bfloat16 [576, 1152], P('seq'), may hold values from -0.25 to 0.25
Outputs:
- hidden_grad: bfloat16 [512, 256, 1152], P(('clip', 'seq')), parts along dimension 0
- spatial_grad: bfloat16 [3, 512, 256, 576], P(None, ('clip', 'seq')), parts along dimension 1
The draws below stay inside these ranges and needn't reach their ends.
There are 8 independent parts, one for each index of `clip`. The reference program is written for one: setup_inputs(seed, part) draws one part's arguments, and reference() takes and returns one part's arrays. A program takes and returns all parts, laid end to end along the dimension named above; an argument that names none is the same for every part. Nothing has to cross between parts.
All inputs are finite; a program needn't handle non-finite values.
Results may differ from the reference program's by a relative error of at most 0.024.
Values may be sent and summed in bfloat16 or wider, within the bound.
A program may use at most 64 MiB of HBM per device.

```python
import math
import jax
import jax.numpy as jnp
from jax import lax

D = 1152
HEADS = 8
HD = 72
PATCH = 256
FRAMES = 64
AW = 576


def draw_spatial_saved(key, part):
    shape = (3, FRAMES, PATCH, HEADS * HD)
    return jnp.clip(jax.random.normal(key, shape, jnp.float32), -4.0, 4.0).astype(jnp.bfloat16)


def draw_modulation(key, part):
    return jax.random.uniform(key, (D,), jnp.float32, -0.5, 0.5)


def level_of(stream_key, dims, cuts, low, top_value):
    factor_of, own = 1.0, jax.random.fold_in(stream_key, 6)
    for dim, parts in cuts:
        heights = jnp.exp(jax.random.uniform(jax.random.fold_in(own, dim), (parts,), jnp.float32, low / len(cuts), top_value / len(cuts)))
        factor_of = factor_of * jnp.repeat(heights, dims[dim] // parts).reshape([-1 if axis == dim else 1 for axis in range(len(dims))])
    return factor_of


def normal_values(own_key, dims, scale, most, shards=(), dtype=jnp.bfloat16):
    values = scale * jax.random.normal(own_key, dims, jnp.float32)
    if shards:
        values = values * level_of(own_key, dims, shards, -0.22, 0.18)
    return jnp.clip(values, -most, most).astype(dtype)


def setup_inputs(seed: int = 0, part: int = 0) -> dict:
    key_of = jax.random.split(jax.random.key(seed), 8)
    part_keys = jax.random.split(jax.random.fold_in(key_of[7], part), 8)
    spatial_saved = draw_spatial_saved(jax.random.fold_in(jax.random.fold_in(key_of[7], part), 71), part)
    hidden = normal_values(part_keys[1], (FRAMES, PATCH, D), 1.0, 6.0, ((0, 64),))
    temporal_out_grad = normal_values(part_keys[2], (FRAMES, PATCH, AW), 1.0, 6.0, ((0, 64),))
    stream_grad = normal_values(part_keys[3], (FRAMES, PATCH, D), 1.0, 6.0, ((0, 64),))
    modulation = draw_modulation(jax.random.fold_in(key_of[7], 71), part)
    temporal_weights = normal_values(key_of[5], (D, 3 * AW), D ** -0.5, 0.1875, ((0, 64),))
    spatial_weights = normal_values(key_of[6], (AW, D), AW ** -0.5, 0.25, ((0, 64),))
    return dict(spatial_saved=spatial_saved, hidden=hidden, temporal_out_grad=temporal_out_grad, stream_grad=stream_grad, modulation=modulation, temporal_weights=temporal_weights, spatial_weights=spatial_weights)


epsilon = 1e-06

def attend_grad(query, keys, values, grad_o, form):
    query = query.astype(jnp.float32)
    keys = keys.astype(jnp.float32)
    values = values.astype(jnp.float32)
    grad_o = grad_o.astype(jnp.float32)
    key_form = form.replace('l', 'm')
    scale = 1.0 / math.sqrt(query.shape[-1])
    scores = jnp.einsum(form + ',' + key_form + '->bhlm', query, keys) * scale
    attention = jax.nn.softmax(scores, axis=-1)
    rounded = attention.astype(jnp.bfloat16).astype(jnp.float32)
    output = jnp.einsum('bhlm,' + key_form + '->' + form, rounded, values)
    delta = jnp.einsum(form + ',' + form + '->bhl', grad_o, output)
    spread = jnp.einsum(form + ',' + key_form + '->bhlm', grad_o, values)
    dscore = (attention * (spread - delta[..., None])).astype(jnp.bfloat16).astype(jnp.float32)
    grad_query = (jnp.einsum('bhlm,' + key_form + '->' + form, dscore, keys) * scale).astype(jnp.bfloat16)
    grad_keys = (jnp.einsum('bhlm,' + form + '->' + key_form, dscore, query) * scale).astype(jnp.bfloat16)
    grad_values = jnp.einsum('bhlm,' + form + '->' + key_form, rounded, grad_o).astype(jnp.bfloat16)
    return (grad_query, grad_keys, grad_values)

def split_heads(block):
    return block.reshape(block.shape[:-1] + (HEADS, HD))

def merge_heads(block):
    return block.reshape(block.shape[:-2] + (HEADS * HD,))

def layer_norm(hidden, modulation):
    widened = hidden.astype(jnp.float32)
    mean_value = lax.optimization_barrier(jnp.mean(widened, axis=-1, keepdims=True))
    centered = widened - mean_value
    inverse = lax.rsqrt(lax.optimization_barrier(jnp.mean(centered * centered, axis=-1, keepdims=True)) + epsilon)
    normal_form = centered * inverse
    normed = (normal_form * (1.0 + modulation.astype(jnp.float32))).astype(jnp.bfloat16)
    return (normed, normal_form, inverse)

def norm_back(grad_normed, normal_form, inverse, modulation):
    scaled = grad_normed * (1.0 + modulation.astype(jnp.float32))
    return inverse * (scaled - lax.optimization_barrier(jnp.mean(scaled, axis=-1, keepdims=True)) - normal_form * lax.optimization_barrier(jnp.mean(scaled * normal_form, axis=-1, keepdims=True)))

def reference(spatial_saved, hidden, temporal_out_grad, stream_grad, modulation, temporal_weights, spatial_weights):
    width = HEADS * HD
    normed, normal_form, inverse = layer_norm(hidden, modulation)
    projected = jnp.dot(normed.reshape(-1, D), temporal_weights, preferred_element_type=jnp.float32)
    projected = projected.astype(jnp.bfloat16).reshape(FRAMES, PATCH, 3 * width)
    grads = attend_grad(split_heads(projected[..., :width]), split_heads(projected[..., width:2 * width]), split_heads(projected[..., 2 * width:]), split_heads(temporal_out_grad), 'lbhd')
    projection_grads = jnp.concatenate([merge_heads(gradient) for gradient in grads], axis=-1)
    norm_grad = jnp.dot(projection_grads.reshape(-1, 3 * width), temporal_weights.T, preferred_element_type=jnp.float32).reshape(FRAMES, PATCH, D)
    branch = norm_back(norm_grad, normal_form, inverse, modulation).astype(jnp.bfloat16)
    branch = lax.optimization_barrier(branch)
    hidden_grad = (stream_grad.astype(jnp.float32) + branch.astype(jnp.float32)).astype(jnp.bfloat16)
    attention_grad = jnp.dot(hidden_grad.reshape(-1, D), spatial_weights.T, preferred_element_type=jnp.float32)
    attention_grad = attention_grad.astype(jnp.bfloat16).reshape(FRAMES, PATCH, width)
    spatial = attend_grad(split_heads(spatial_saved[0]), split_heads(spatial_saved[1]), split_heads(spatial_saved[2]), split_heads(attention_grad), 'blhd')
    spatial_grad = jnp.stack([merge_heads(gradient) for gradient in spatial])
    return (hidden_grad, spatial_grad)
```

```python
import functools
import math
import jax, jax.numpy as jnp
from jax import lax
from jax.experimental import pallas as pl
from jax.sharding import PartitionSpec as P
from jax.experimental.pallas import tpu as pltpu
HEADS=8; HD=72; AW=576
SCALE=1.0/math.sqrt(HD)
F32=jnp.float32; BF=jnp.bfloat16
NT=(((1,),(1,)),((),()))
TN=(((0,),(0,)),((),()))
NN=(((1,),(0,)),((),()))
def dot(a,b,dims): return lax.dot_general(a,b,dims,preferred_element_type=F32)

def windows():
    out=[]
    for h in range(HEADS):
        lo=72*h; hi=lo+72
        s=(lo//128)*128; e=-(-hi//128)*128
        e=min(e,AW)
        out.append((lo,hi,s,e))
    return out

def attend(q_ref,k_ref,v_ref,g_ref,dq_ref,dk_ref,dv_ref,mask):
    for r in (dq_ref,dk_ref,dv_ref):
        r[...]=jnp.zeros_like(r)
    for lo,hi,s,e in windows():
        lane=lax.broadcasted_iota(jnp.int32,(256,e-s),1)+s
        sel=(lane>=lo)&(lane<hi)
        def pick(r): return jnp.where(sel,r[:,s:e].astype(F32),0.0).astype(BF)
        q=pick(q_ref); k=pick(k_ref); v=pick(v_ref); g=pick(g_ref)
        sc=dot(q,k,NT)*SCALE
        if mask is not None: sc=jnp.where(mask,sc,-1e30)
        m=jnp.max(sc,axis=1,keepdims=True)
        p=jnp.exp(sc-m)
        p=p*(1.0/jnp.sum(p,axis=1,keepdims=True))
        pb=p.astype(BF)
        spread=dot(g,v,NT)
        delta=jnp.sum(pb.astype(F32)*spread,axis=1,keepdims=True)
        ds=(p*(spread-delta)).astype(BF)
        dq_ref[:,s:e]+=dot(ds,k,NN)
        dk_ref[:,s:e]+=dot(ds,q,TN)
        dv_ref[:,s:e]+=dot(pb,g,TN)

def temporal_kernel(h_ref,g_ref,w_ref,mod_ref,out_ref,wq,wk,wv,hf,gf,q_s,k_s,v_s,dq,dk,dv):
    for b in range(8):
        for n,dst in enumerate((wq,wk,wv)):
            parts=[w_ref[8*b+i,18*n:18*n+18,:].astype(F32) for i in range(8)]
            dst[144*b:144*b+144,:]=jnp.concatenate(parts,axis=0).astype(BF)
    for f in range(64):
        hf[4*f:4*f+4,:]=h_ref[f].astype(F32)
        gf[4*f:4*f+4,:]=g_ref[f].astype(F32)
    x=hf[...]
    mean=jnp.mean(x,axis=1,keepdims=True)
    cen=x-mean
    inv=lax.rsqrt(jnp.mean(cen*cen,axis=1,keepdims=True)+1e-6)
    one=1.0+mod_ref[...]
    nf=cen*inv
    normed=(nf*one).astype(BF)
    q_s[...]=dot(normed,wq[...],NN).astype(BF)
    k_s[...]=dot(normed,wk[...],NN).astype(BF)
    v_s[...]=dot(normed,wv[...],NN).astype(BF)
    i=lax.broadcasted_iota(jnp.int32,(256,256),0)
    j=lax.broadcasted_iota(jnp.int32,(256,256),1)
    mask=((i-j)&3)==0
    attend(q_s,k_s,v_s,gf,dq,dk,dv,mask)
    ng=dot((dq[...]*SCALE).astype(BF),wq[...],NT)
    ng+=dot((dk[...]*SCALE).astype(BF),wk[...],NT)
    ng+=dot(dv[...].astype(BF),wv[...],NT)
    s=ng*one
    nf=(hf[...]-mean)*inv
    br=inv*(s-jnp.mean(s,axis=1,keepdims=True)-nf*jnp.mean(s*nf,axis=1,keepdims=True))
    hf[...]=br
    for f in range(64):
        out_ref[f]=hf[4*f:4*f+4,:].astype(BF)

def spatial_kernel(br_ref,st_ref,sv_ref,w_ref,hg_ref,sg_ref,ws,bf,g_s,dq,dk,dv):
    for b in range(4):
        for n in range(9):
            parts=[w_ref[16*b+i,9*n:9*n+9,:].astype(F32) for i in range(16)]
            ws[144*b:144*b+144,128*n:128*n+128]=jnp.concatenate(parts,axis=0).astype(BF)
    for f in range(64):
        bf[4*f:4*f+4,:]=br_ref[f].astype(F32)
    hg=(st_ref[0].astype(F32)+bf[...]).astype(BF)
    hg_ref[0]=hg
    g_s[...]=dot(hg,ws[...],NT).astype(BF)
    attend(sv_ref.at[0,0],sv_ref.at[1,0],sv_ref.at[2,0],g_s,dq,dk,dv,None)
    sg_ref[0,0]=(dq[...]*SCALE).astype(BF)
    sg_ref[1,0]=(dk[...]*SCALE).astype(BF)
    sg_ref[2,0]=dv[...].astype(BF)

V=lambda *s,d=F32: pltpu.VMEM(s,d)
VS=pl.BlockSpec(memory_space=pltpu.VMEM)
def temporal(h,g,w,mod):
    return pl.pallas_call(temporal_kernel,out_shape=jax.ShapeDtypeStruct((64,4,1152),BF),
        in_specs=[VS]*4,out_specs=VS,
        scratch_shapes=[V(1152,576,d=BF)]*3+[V(256,1152),V(256,576)]+[V(256,576,d=BF)]*3+[V(256,576)]*3,
        compiler_params=pltpu.CompilerParams(vmem_limit_bytes=60<<20))(h,g,w,mod)
def spatial(br,st,sv,w):
    return pl.pallas_call(spatial_kernel,out_shape=(jax.ShapeDtypeStruct((1,256,1152),BF),jax.ShapeDtypeStruct((3,1,256,576),BF)),
        in_specs=[VS]*4,out_specs=(VS,VS),
        scratch_shapes=[V(576,1152,d=BF),V(256,1152),V(256,576,d=BF)]+[V(256,576)]*3,
        compiler_params=pltpu.CompilerParams(vmem_limit_bytes=60<<20))(br,st,sv,w)

MESH=pl.DeviceIdType.MESH
DYS=(1,7,2,6,3,5,4)

def exchange_kernel(n_a2a, *refs):
    srcs=refs[:n_a2a]; shard=refs[n_a2a]
    dsts=refs[n_a2a+1:2*n_a2a+1]; W=refs[2*n_a2a+1]
    (a_s,a_r,z_s,z_r,y_s,y_r,x_s,x_r,c_s,c_r,l_s)=refs[2*n_a2a+2:]
    clip=lax.axis_index("clip"); seq=lax.axis_index("seq")
    x=lax.rem(clip,4); x0=clip-x
    y=lax.div(seq,8); zc=lax.rem(seq,8); z=lax.div(zc,2); c=lax.rem(zc,2)

    def to(clip_,seq_): return {"clip":clip_,"seq":seq_}
    def rc(src,dst,ss,rs,clip_,seq_):
        return pltpu.make_async_remote_copy(src_ref=src,dst_ref=dst,send_sem=ss,recv_sem=rs,
            device_id=to(clip_,seq_),device_id_type=MESH)
    def row(dy): return lax.rem(y+dy,8)
    def col(dx): return x0+lax.rem(x+dx,4)
    def held(y_,x_,c_): return y_*8+lax.rem(x_-y_+8,4)*2+c_

    barrier=pltpu.get_barrier_semaphore()
    @pl.loop(1,64)
    def _(k): pl.semaphore_signal(barrier,inc=1,device_id=to(clip,lax.rem(seq+k,64)),device_id_type=MESH)
    for dx in (1,2,3):
        pl.semaphore_signal(barrier,inc=1,device_id=to(col(dx),seq),device_id_type=MESH)
    pl.semaphore_wait(barrier,66)

    def a2a_copy(a,dy,j):
        d=row(dy)*8+lax.rem(zc+j,8)
        return rc(srcs[a].at[d],dsts[a].at[seq],a_s.at[a,dy,j],a_r.at[a,dy,j],clip,d)
    def a2a_from(a,dy,j):
        d=row(8-dy)*8+lax.rem(zc-j+8,8)
        return rc(srcs[a].at[d],dsts[a].at[d],a_s.at[a,dy,j],a_r.at[a,dy,j],clip,d)
    def send_rows(dy,lo):
        @pl.loop(lo,8)
        def _(j):
            for a in range(n_a2a): a2a_copy(a,dy,j).start()

    src=held(y,x,c)
    is_src=z==lax.rem(x-y+8,4)
    @pl.when(is_src)
    def _():
        for dz in (1,2,3):
            rc(shard,W.at[src],z_s.at[dz-1],z_r,clip,y*8+lax.rem(z+dz,4)*2+c).start()
        pltpu.make_async_copy(shard,W.at[src],l_s.at[n_a2a]).start()
    send_rows(0,1)
    for a in range(n_a2a):
        pltpu.make_async_copy(srcs[a].at[seq],dsts[a].at[seq],l_s.at[a]).start()
    @pl.when(is_src)
    def _():
        pltpu.make_async_copy(shard,W.at[src],l_s.at[n_a2a]).wait()
    @pl.when(jnp.logical_not(is_src))
    def _():
        rc(shard,W.at[src],z_s.at[0],z_r,clip,seq).wait_recv()
    def y_copy(dy): return rc(W.at[src],W.at[src],y_s.at[dy],y_r.at[dy],clip,row(dy)*8+zc)
    def y_from(dy):
        i=held(row(8-dy),x,c)
        return rc(W.at[i],W.at[i],y_s.at[dy],y_r.at[dy],clip,row(8-dy)*8+zc)
    def x_copy(dy,dx):
        i=held(row(8-dy),x,c)
        return rc(W.at[i],W.at[i],x_s.at[dy,dx],x_r.at[dy,dx],col(dx),seq)
    def x_from(dy,dx):
        i=held(row(8-dy),lax.rem(x-dx+4,4),c)
        return rc(W.at[i],W.at[i],x_s.at[dy,dx],x_r.at[dy,dx],col(4-dx),seq)
    peer=seq+1-2*c
    def c_copy(dy,dx):
        i=held(row(8-dy),lax.rem(x-dx+4,4),c)
        return rc(W.at[i],W.at[i],c_s.at[dy,dx],c_r.at[dy,dx],clip,peer)
    def c_from(dy,dx):
        i=held(row(8-dy),lax.rem(x-dx+4,4),1-c)
        return rc(W.at[i],W.at[i],c_s.at[dy,dx],c_r.at[dy,dx],clip,peer)
    for dy in DYS: y_copy(dy).start()
    def forward(dy):
        for dx in (1,3,2): x_copy(dy,dx).start()
        c_copy(dy,0).start()
    forward(0)
    for dy in DYS: send_rows(dy,0)
    for dy in DYS:
        y_from(dy).wait_recv()
        forward(dy)
    for dy in (0,)+DYS:
        for dx in (1,3,2):
            x_from(dy,dx).wait_recv()
            c_copy(dy,dx).start()
    for dy in range(8):
        for dx in range(4):
            c_from(dy,dx).wait_recv()
    def drain(dy,lo):
        @pl.loop(lo,8)
        def _(j):
            for a in range(n_a2a):
                a2a_from(a,dy,j).wait_recv()
                a2a_copy(a,dy,j).wait_send()
    drain(0,1)
    for dy in DYS: drain(dy,0)
    for dy in range(8):
        if dy: y_copy(dy).wait_send()
        for dx in range(4):
            if dx: x_copy(dy,dx).wait_send()
            c_copy(dy,dx).wait_send()
    @pl.when(is_src)
    def _():
        for dz in (1,2,3):
            rc(shard,W.at[src],z_s.at[dz-1],z_r,clip,y*8+lax.rem(z+dz,4)*2+c).wait_send()
    for a in range(n_a2a):
        pltpu.make_async_copy(srcs[a].at[seq],dsts[a].at[seq],l_s.at[a]).wait()

def exchange(slabs,shard,cid):
    n=len(slabs)
    DMA=pltpu.SemaphoreType.DMA
    A=pl.BlockSpec(memory_space=pl.ANY)
    return pl.pallas_call(functools.partial(exchange_kernel,n),
        out_shape=tuple(jax.ShapeDtypeStruct(s.shape,s.dtype) for s in slabs)+(jax.ShapeDtypeStruct((64,)+shard.shape,shard.dtype),),
        in_specs=[A]*(n+1),out_specs=(A,)*(n+1),
        scratch_shapes=[DMA((n,8,8)),DMA((n,8,8)),DMA((3,)),DMA,DMA((8,)),DMA((8,)),DMA((8,4)),DMA((8,4)),DMA((8,4)),DMA((8,4)),DMA((n+1,))],
        compiler_params=pltpu.CompilerParams(collective_id=cid,has_side_effects=True))(*slabs,shard)

def shards(spatial_saved,hidden,temporal_out_grad,stream_grad,modulation,temporal_weights,spatial_weights):
    hs=hidden.reshape(64,4,1152)
    gs=temporal_out_grad.reshape(64,4,576)
    tw=jnp.concatenate([temporal_weights[:,0:576],temporal_weights[:,576:1152],temporal_weights[:,1152:]],axis=0)
    sw=spatial_weights.reshape(9,9,128).transpose(1,0,2).reshape(81,128)
    hr,gr,W=exchange((hs,gs),tw,0)
    branch=temporal(hr,gr,W,modulation.reshape(1,1152))
    br,S=exchange((branch,),sw,1)
    return spatial(br,stream_grad,spatial_saved,S)

def solution(mesh):
    return jax.shard_map(shards,mesh=mesh,
        in_specs=(P(None,("clip","seq"),None,None),P(("clip","seq"),None,None),P(("clip","seq"),None,None),P(("clip","seq"),None,None),P(),P("seq",None),P("seq",None)),
        out_specs=(P(("clip","seq"),None,None),P(None,("clip","seq"),None,None)),check_vma=False)
```
